32 devices in a mesh: wide: 16 (over z, y, core), narrow: 2 (over x).
Axes of the slice: x: 2, y: 2, z: 4, core: 2. Of those that a mesh axis runs over, the one named last changes fastest.
Arguments:
- gradient: float32 [3072, 3072], P('wide', 'narrow'), may hold values from -6 to 6
- first_moment: float32 [3072, 3072], P('wide', 'narrow'), may hold values from -6 to 6
- second_moment: float32 [3072, 3072], P('wide', 'narrow'), may hold values from 0.25 to 4
- left_basis: float32 [3072, 3072], P('wide', 'narrow'), may hold values from -0.15625 to 0.15625
- right_basis: float32 [3072, 3072], P('wide', 'narrow'), may hold values from -0.109375 to 0.109375
Outputs:
- update: float32 [3072, 3072], P('wide', 'narrow')
- new_first: float32 [3072, 3072], P('wide', 'narrow')
- new_second: float32 [3072, 3072], P('wide', 'narrow')
The draws below stay inside these ranges and needn't reach their ends.
All inputs are finite; a program needn't handle non-finite values.
Results may differ from the reference program's by a relative error of at most 0.000075.
Values sent between devices are 32-bit elements; how exact they have to be, the bound alone decides.
A program may use at most 128 MiB of HBM per device.

```python
import math
import jax
import jax.numpy as jnp
from jax import lax

M = 3072
N = 3072
STEP = 10


def strengthened(drawn, stream_key, source, target, blocks, factor):
    def block_of(position):
        return (jnp.arange(drawn.shape[position]) // (drawn.shape[position] // blocks)).reshape((-1,) + (1,) * (drawn.ndim - 1 - position))

    first = jax.random.permutation(stream_key, blocks)[block_of(target)]
    far = (block_of(target) + blocks // 2) % blocks
    return jnp.where((block_of(source) == first) | (block_of(source) == far), factor * drawn, drawn)


def shard_levels(own_key, dims, cuts, low, high):
    gain = 1.0
    for dim, parts in cuts:
        steps = jax.random.uniform(jax.random.fold_in(jax.random.fold_in(own_key, 6), dim), (parts,), jnp.float32, low / len(cuts), high / len(cuts))
        gain = gain * jnp.repeat(jnp.exp(steps), dims[dim] // parts).reshape((-1,) + (1,) * (len(dims) - 1 - dim))
    return gain


def bell_draw(own_key, dims, scale, bound, cuts=(), held_as=jnp.bfloat16):
    values = scale * jax.random.normal(own_key, dims, jnp.float32)
    if cuts:
        values = values * shard_levels(own_key, dims, cuts, -0.22, 0.18)
    return jnp.clip(values, -bound, bound).astype(held_as)


def heavy_noise(key, dims, scale, most, shards, heavy, held_as=jnp.bfloat16):
    values = scale * jax.random.normal(key, dims, jnp.float32)
    if shards:
        values = values * shard_levels(key, dims, shards, -0.22, 0.18)
    return jnp.clip(strengthened(values, jax.random.fold_in(key, 3), *heavy), -most, most).astype(held_as)


def setup_inputs(seed: int = 0) -> dict:
    splits = jax.random.split(jax.random.key(seed), 6)
    return {
        "gradient": bell_draw(splits[0], (M, N), 1.0, 6.0, ((0, 16), (1, 2)), jnp.float32),
        "first_moment": bell_draw(splits[1], (M, N), 1.0, 6.0, ((0, 16), (1, 2)), jnp.float32),
        "second_moment": jnp.clip(jnp.exp(math.log(4.0) - 2.7725887 * jax.random.uniform(splits[2], (M, N), jnp.float32) ** shard_levels(splits[2], (M, N), ((0, 16), (1, 2)), -0.2, 0.2)), 0.25, 4.0),
        "left_basis": heavy_noise(splits[3], (M, M), M ** -0.5, 0.15625, ((0, 16), (1, 2)), (0, 1, 16, 2.0), jnp.float32),
        "right_basis": bell_draw(splits[4], (N, N), N ** -0.5, 0.109375, ((0, 16), (1, 2)), jnp.float32),
    }


beta_first = 0.9
beta_second = 0.95
epsilon = 1e-08

def product(left, right):
    return jnp.dot(left, right, precision=lax.Precision.HIGHEST, preferred_element_type=jnp.float32)

def reference(gradient, first_moment, second_moment, left_basis, right_basis):
    rotated_right = product(gradient, right_basis)
    rotated = product(left_basis.T, rotated_right)
    new_first = beta_first * first_moment + (1.0 - beta_first) * rotated
    new_second = beta_second * second_moment + (1.0 - beta_second) * rotated * rotated
    direction = new_first / (1.0 - beta_first ** STEP) / (jnp.sqrt(new_second / (1.0 - beta_second ** STEP)) + epsilon)
    back_left = product(left_basis, direction)
    update = product(back_left, right_basis.T)
    return (update, new_first, new_second)
```

```python
import jax
import jax.numpy as jnp
from jax import lax
from jax.sharding import PartitionSpec as P

STEP = 10


beta_first = 0.9
beta_second = 0.95
epsilon = 1e-08


CHUNKS = 2


def contract(left, right, left_dim, right_dim):
    return lax.dot_general(
        left,
        right,
        (((left_dim,), (right_dim,)), ((), ())),
        precision=lax.Precision.HIGH,
        preferred_element_type=jnp.float32,
    )


def whole_rows(block):
    if lax.axis_size("narrow") != 2:
        return lax.all_gather(block, "narrow", axis=1, tiled=True)
    other = lax.ppermute(block, "narrow", ((0, 1), (1, 0)))
    first = lax.axis_index("narrow") == 0
    return jnp.concatenate(
        (jnp.where(first, block, other), jnp.where(first, other, block)), axis=1
    )


def body(gradient, first_moment, second_moment, left_basis, right_basis):
    width = gradient.shape[1] // CHUNKS
    parts = [slice(k * width, (k + 1) * width) for k in range(CHUNKS)]
    panel = lambda block: lax.all_gather(block, "wide", axis=0, tiled=True)

    left_rows = whole_rows(left_basis)
    grad_rows = whole_rows(gradient)
    left_columns = lax.all_to_all(left_rows, "wide", split_axis=1, concat_axis=0, tiled=True)

    rights = [panel(right_basis[:, part]) for part in parts]
    rotated_rights = [panel(contract(grad_rows, right, 1, 0)) for right in rights]
    firsts, seconds, terms = [], [], 0.0
    for part, right, rotated_right in zip(parts, rights, rotated_rights):
        rotated = contract(left_columns, rotated_right, 0, 0)
        new_first = beta_first * first_moment[:, part] + (1.0 - beta_first) * rotated
        new_second = beta_second * second_moment[:, part] + (1.0 - beta_second) * rotated * rotated
        direction = (
            new_first
            / (1.0 - beta_first**STEP)
            / (jnp.sqrt(new_second / (1.0 - beta_second**STEP)) + epsilon)
        )
        back_left = contract(left_rows, panel(direction), 1, 0)
        terms = terms + contract(back_left, right, 1, 1)
        firsts.append(new_first)
        seconds.append(new_second)
    update = lax.psum_scatter(terms, "narrow", scatter_dimension=1, tiled=True)
    return (update, jnp.concatenate(firsts, axis=1), jnp.concatenate(seconds, axis=1))


def solution(mesh):
    placed = (
        P("wide", "narrow"),
        P("wide", "narrow"),
        P("wide", "narrow"),
        P("wide", "narrow"),
        P("wide", "narrow"),
    )
    return jax.shard_map(
        body,
        mesh=mesh,
        in_specs=placed,
        out_specs=(P("wide", "narrow"), P("wide", "narrow"), P("wide", "narrow")),
        check_vma=False,
    )
```
